256 devices in a mesh: energy: 32 (over x_hi, z, core), seg: 8 (over x_lo, y).
Axes of the slice: x: 4 (x_hi: 2, x_lo: 2; x = x_hi * 2 + x_lo), y: 4, z: 8, core: 2. Of those that a mesh axis runs over, the one named last changes fastest.
Arguments:
- onsite: float32 [8, 384, 384], P('seg'), may hold values from -3 to 8
- coupling: float32 [8, 384, 384], P('seg'), may hold values from -2 to 2
- phonon: float32 [8, 384, 384], P('seg'), may hold values from -1 to 1
- levels: float32 [32], P('energy'), may hold values from 0.5 to 2
- offsets: int32 [2], replicated, may hold values from 1 to 15
Outputs:
- green_fn: float32 [32, 8, 384, 384], P('energy', 'seg')
- self_energy: float32 [32, 8, 384, 384], P('energy', 'seg')
The draws below stay inside these ranges and needn't reach their ends.
All inputs are finite; a program needn't handle non-finite values.
Results may differ from the reference program's by a relative error of at most 0.0001.
Values sent between devices are 32-bit elements; how exact they have to be, the bound alone decides.
A program may use at most 64 MiB of HBM per device.

```python
import math
import jax
import jax.numpy as jnp
from jax import lax

NB = 384
NS = 4
BORN = 2
NE = 32
SEGS = 8


def draw_onsite(key, part):
    first_key, second_key = jax.random.split(jax.random.fold_in(key, 11))
    identity = jnp.eye(NB, dtype=jnp.float32)
    diagonal_part = jax.random.uniform(first_key, (SEGS, NB, 1), jnp.float32, 3.0, 5.0)
    scatter_part = jnp.clip(jax.random.normal(second_key, (SEGS, NB, NB), jnp.float32), -6.0, 6.0) * (2.6 / NB ** 0.5)
    return scatter_part + diagonal_part * identity


def draw_coupling(key, part):
    inner_key = jax.random.fold_in(key, 23)
    values = jnp.clip(jax.random.normal(inner_key, (SEGS, NB, NB), jnp.float32), -6.0, 6.0) * (1.2 / NB ** 0.5)
    return values


def draw_phonon(key, part):
    inner_key = jax.random.fold_in(key, 37)
    values = jnp.clip(jax.random.normal(inner_key, (SEGS, NB, NB), jnp.float32), -6.0, 6.0) * (0.7 / NB ** 0.5)
    return values


def block_levels(rng, dims, cuts, least, top_value):
    factor_of, own = 1.0, jax.random.fold_in(rng, 6)
    for axis_at, parts in cuts:
        draws = jnp.exp(jax.random.uniform(jax.random.fold_in(own, axis_at), (parts,), jnp.float32, least / len(cuts), top_value / len(cuts)))
        factor_of = factor_of * jnp.repeat(draws, dims[axis_at] // parts).reshape([-1 if axis == axis_at else 1 for axis in range(len(dims))])
    return factor_of


def setup_inputs(seed: int = 0) -> dict:
    key_list = jax.random.split(jax.random.key(seed), 6)
    onsite = draw_onsite(jax.random.fold_in(key_list[5], 71), 0)
    coupling = draw_coupling(jax.random.fold_in(key_list[5], 71), 0)
    phonon = draw_phonon(jax.random.fold_in(key_list[5], 71), 0)
    levels = jnp.clip(jnp.exp(math.log(2.0) - 1.3862944 * jax.random.uniform(key_list[3], (NE,), jnp.float32) ** block_levels(key_list[3], (NE,), ((0, 32),), -0.2, 0.2)), 0.5, 2.0)
    offsets = jax.random.randint(key_list[4], (2,), 1, 16).astype(jnp.int32)
    return {"onsite": onsite, "coupling": coupling, "phonon": phonon, "levels": levels, "offsets": offsets}


def product(left_block, right_block):
    return jnp.matmul(left_block, right_block, precision=lax.Precision.HIGHEST)


def transpose(matrix):
    return jnp.swapaxes(matrix, -1, -2)


def invert(matrix):
    order_size = matrix.shape[-1]
    identity = jnp.eye(order_size, dtype=jnp.float32)
    approx = identity / jnp.diagonal(matrix, axis1=-2, axis2=-1)[..., None, :]
    for sweep_index in range(NS):
        approx = product(approx, 2.0 * identity - product(matrix, approx))
    return approx


def dyson_sweep(onsite, coupling, levels, self_energy):
    seg_total = onsite.shape[0]
    identity = jnp.eye(onsite.shape[-1], dtype=jnp.float32)
    lead_term = product(coupling[0], transpose(coupling[0])) * 0.25
    left_list = []
    for segment in range(seg_total):
        matrix = onsite[segment] + levels[:, None, None] * identity + self_energy[:, segment]
        if segment == 0:
            inner_term = lead_term
        else:
            inner_term = product(product(coupling[segment], left_list[-1]), transpose(coupling[segment]))
        left_list.append(invert(matrix - inner_term))
    full_blocks = [None] * seg_total
    full_blocks[seg_total - 1] = left_list[seg_total - 1]
    for segment in range(seg_total - 2, -1, -1):
        next_coupling = coupling[segment + 1]
        weight_in = product(product(transpose(next_coupling), full_blocks[segment + 1]), next_coupling)
        left_block = left_list[segment]
        full_blocks[segment] = left_block + product(product(left_block, weight_in), left_block)
    return jnp.stack(full_blocks, axis=1)


def shifted(field, amount):
    count_energy = field.shape[0]
    positions = jnp.arange(count_energy, dtype=jnp.int32)
    source = (positions - amount).astype(jnp.int32)
    inside = ((source >= 0) & (source < count_energy)).astype(jnp.float32)
    gathered = jnp.take(field, jnp.clip(source, 0, count_energy - 1).astype(jnp.int32), axis=0)
    return gathered * inside[:, None, None, None]


def phonon_term(green_fn, phonon, offsets):
    combined = shifted(green_fn, offsets[0]) + shifted(green_fn, offsets[1])
    combined = combined + shifted(green_fn, -offsets[0]) + shifted(green_fn, -offsets[1])
    return product(product(phonon[None], combined), transpose(phonon)[None])


def reference(onsite, coupling, phonon, levels, offsets):
    self_energy = jnp.zeros((levels.shape[0],) + onsite.shape, dtype=jnp.float32)
    green_fn = self_energy
    for round_index in range(BORN):
        green_fn = dyson_sweep(onsite, coupling, levels, self_energy)
        if round_index < BORN - 1:
            self_energy = phonon_term(green_fn, phonon, offsets)
    return green_fn, self_energy
```

```python
import functools, jax, jax.numpy as jnp
from jax import lax
from jax.experimental import pallas as pl
from jax.experimental.pallas import tpu as pltpu
NB=384
f32=jnp.float32; bf16=jnp.bfloat16

def split(x):
    hi = x.astype(bf16)
    lo = (x - hi.astype(f32)).astype(bf16)
    return hi, lo

def put(ref, x):
    hi, lo = split(x)
    ref[0] = hi
    ref[1] = lo

def put_at(ref, i, x):
    hi, lo = split(x)
    ref[i, 0] = hi
    ref[i, 1] = lo

def dot(a, b):
    return lax.dot_general(a, b, (((1,), (0,)), ((), ())), preferred_element_type=f32)

def dott(a, b):
    return lax.dot_general(a, b, (((1,), (1,)), ((), ())), preferred_element_type=f32)

def mm(a, b, d=dot):
    ah, al = a; bh, bl = b
    return d(ah, bh) + (d(ah, bl) + d(al, bh))

def rd(ref):
    return ref[0], ref[1]
def rd_at(ref, i):
    return ref[i, 0], ref[i, 1]

def chain_kernel(sref, lev_ref, m_ref, c_ref, o_ref, L, P, Q, C, e_s, r_s, b_s, g_s):
    seg = sref[0]
    row = lax.broadcasted_iota(jnp.int32, (NB, NB), 0)
    col = lax.broadcasted_iota(jnp.int32, (NB, NB), 1)
    eye = (row == col).astype(f32)
    lev = lev_ref[0]

    def inv_into(x, s):
        diag = x * eye
        d_row = 1.0 / jnp.sum(diag, axis=0, keepdims=True)
        d_col = 1.0 / jnp.sum(diag, axis=1, keepdims=True)
        e = eye - x * d_row
        put(e_s, e)
        b = eye + e
        r = mm(rd(e_s), rd(e_s))
        put(r_s.at[0], r)
        put(b_s, b)
        b = b + mm(rd(r_s.at[0]), rd(b_s))
        r = mm(rd(r_s.at[0]), rd(r_s.at[0]))
        put(r_s.at[1], r)
        put(b_s, b)
        b = b + mm(rd(r_s.at[1]), rd(b_s))
        r = mm(rd(r_s.at[1]), rd(r_s.at[1]))
        put(r_s.at[0], r)
        put(b_s, b)
        b = b + mm(rd(r_s.at[0]), rd(b_s))
        L[s] = b * d_col

    put_at(C, 0, c_ref[0])
    x0 = m_ref[0] + lev * eye - 0.25 * mm(rd_at(C, 0), rd_at(C, 0), dott)
    inv_into(x0, 0)

    def fwd(s, _):
        put_at(C, s, c_ref[s])
        put(b_s, L[s - 1])
        c = rd_at(C, s)
        q = mm(c, rd(b_s))
        put_at(Q, s, q)
        x = m_ref[s] + lev * eye - mm(rd_at(Q, s), c, dott)
        p = mm(rd(b_s), c, dott)
        put_at(P, s, p)
        inv_into(x, s)
        return 0
    lax.fori_loop(1, 8, fwd, 0)

    o_ref[...] = L[7]
    def bwd(k, _):
        t = 6 - k
        put(g_s, o_ref[...])
        pg = mm(rd_at(P, t + 1), rd(g_s))
        put(e_s, pg)
        o_ref[...] = L[t] + mm(rd(e_s), rd_at(Q, t + 1))
        return 0
    lax.fori_loop(0, 7 - seg, bwd, 0)

def chain(seg, lev, m, c):
    nst = m.shape[0]
    vm = pl.BlockSpec(memory_space=pltpu.VMEM)
    sm = pl.BlockSpec(memory_space=pltpu.SMEM)
    return pl.pallas_call(
        chain_kernel, out_shape=jax.ShapeDtypeStruct((NB, NB), f32),
        in_specs=[sm, sm, vm, vm], out_specs=vm,
        scratch_shapes=[pltpu.VMEM((8, NB, NB), f32), pltpu.VMEM((8, 2, NB, NB), bf16), pltpu.VMEM((8, 2, NB, NB), bf16),
                        pltpu.VMEM((8, 2, NB, NB), bf16),
                        pltpu.VMEM((2, NB, NB), bf16), pltpu.VMEM((2, 2, NB, NB), bf16), pltpu.VMEM((2, NB, NB), bf16),
                        pltpu.VMEM((2, NB, NB), bf16)],
        compiler_params=pltpu.CompilerParams(vmem_limit_bytes=60 << 20),
        name="chain",
    )(seg, lev, m, c)


def gathered(block, axis):
    return lax.all_gather(block, axis, axis=0, tiled=False)


def phonon_kernel(phi_ref, comb_ref, o_ref):
    phi = split(phi_ref[...])
    half = mm(phi, split(comb_ref[...]))
    o_ref[...] = mm(split(half), phi, dott)


def phonon_product(phi, comb):
    vm = pl.BlockSpec(memory_space=pltpu.VMEM)
    return pl.pallas_call(
        phonon_kernel, out_shape=jax.ShapeDtypeStruct((NB, NB), f32),
        in_specs=[vm, vm], out_specs=vm, name="phonon_product",
        compiler_params=pltpu.CompilerParams(vmem_limit_bytes=60 << 20),
    )(phi, comb)


def energy_sum(green, offsets):
    count = lax.axis_size("energy")
    rows = NB // count
    pieces = lax.all_to_all(green.reshape(count, rows, NB), "energy", 0, 0, tiled=True)
    reach = count // 2
    padded = jnp.pad(pieces, ((reach, reach), (0, 0), (0, 0)))

    def moved(amount):
        return lax.dynamic_slice_in_dim(padded, reach - amount, count, 0)

    combined = moved(offsets[0]) + moved(offsets[1]) + moved(-offsets[0]) + moved(-offsets[1])
    return lax.all_to_all(combined, "energy", 0, 0, tiled=True).reshape(NB, NB)


def shards(onsite, coupling, phonon, levels, offsets):
    seg = lax.axis_index("seg").astype(jnp.int32).reshape(1)
    onsite_all = gathered(onsite[0], "seg")
    coupling_all = gathered(coupling[0], "seg")
    green = chain(seg, levels, onsite_all, coupling_all)
    self_energy = phonon_product(phonon[0], energy_sum(green, offsets))
    green = chain(seg, levels, onsite_all + gathered(self_energy, "seg"), coupling_all)
    return green[None, None], self_energy[None, None]


def solution(mesh):
    P = jax.sharding.PartitionSpec
    in_specs = (P("seg", None, None), P("seg", None, None), P("seg", None, None), P("energy"), P())
    out_specs = (P("energy", "seg", None, None), P("energy", "seg", None, None))
    return jax.shard_map(shards, mesh=mesh, in_specs=in_specs, out_specs=out_specs, check_vma=False)
```

```python
import functools
import jax
import jax.numpy as jnp
from jax import lax
from jax.experimental import pallas as pl
from jax.experimental.pallas import tpu as pltpu

NB = 384
SEGS = 8
f32 = jnp.float32
bf16 = jnp.bfloat16
MESH = pl.DeviceIdType.MESH


def split(x):
    hi = x.astype(bf16)
    lo = (x - hi.astype(f32)).astype(bf16)
    return hi, lo


def put(ref, x):
    hi, lo = split(x)
    ref[0] = hi
    ref[1] = lo


def rd(ref):
    return ref[0], ref[1]


def dot(a, b):
    return lax.dot_general(a, b, (((1,), (0,)), ((), ())), preferred_element_type=f32)


def dott(a, b):
    return lax.dot_general(a, b, (((1,), (1,)), ((), ())), preferred_element_type=f32)


def mm(a, b, d=dot):
    ah, al = a
    bh, bl = b
    return d(ah, bh) + (d(ah, bl) + d(al, bh))


def table(seg, values):
    out = jnp.int32(values[-1])
    for i, v in enumerate(values[:-1]):
        out = jnp.where(seg == i, jnp.int32(v), out)
    return out


class Gather:
    def __init__(self, bufs, rsem, psem, ssem, dsem, dssem, halves):
        self.bufs, self.rsem, self.psem, self.ssem, self.dsem, self.dssem = bufs, rsem, psem, ssem, dsem, dssem
        e = lax.axis_index("energy")
        self.seg = lax.axis_index("seg")
        core = e % 2
        self.sibling = {"energy": e + 1 - 2 * core}
        pair, y = self.seg // 4, self.seg % 4
        at = lambda p, dy: p * 4 + (y + dy) % 4
        self.up, self.down, self.two = at(pair, 1), at(pair, 3), at(pair, 2)
        self.cross, self.cup, self.cdown, self.ctwo = at(1 - pair, 0), at(1 - pair, 1), at(1 - pair, 3), at(1 - pair, 2)
        self.halves = halves
        n = NB // 2 if halves else NB
        base = core * n if halves else 0
        self.rows = pl.ds(pl.multiple_of(base, 8), n)
        self.low = pl.ds(pl.multiple_of(base, 8), n // 2)
        self.high = pl.ds(pl.multiple_of(base + n // 2, 8), n // 2)

    def copy(self, a, block, rows, s, sem, to):
        ref = self.bufs[a].at[block, rows]
        return pltpu.make_async_remote_copy(
            src_ref=ref, dst_ref=ref, send_sem=self.ssem.at[a, s], recv_sem=sem,
            device_id=to, device_id_type=MESH)

    def got(self, a, block, rows, sem):
        self.copy(a, block, rows, 0, sem, {"seg": self.up}).wait_recv()

    def send(self, a, i):
        r, p = self.rsem, self.psem
        up, down, cross = {"seg": self.up}, {"seg": self.down}, {"seg": self.cross}
        block, rows, sem, to = (
            (self.seg, self.rows, r.at[a, self.seg], up),
            (self.seg, self.rows, r.at[a, self.seg], down),
            (self.seg, self.rows, r.at[a, self.seg], cross),
            (self.down, self.low, p.at[a, 0], up),
            (self.up, self.high, p.at[a, 1], down),
            (self.cross, self.rows, r.at[a, self.cross], up),
            (self.cross, self.rows, r.at[a, self.cross], down),
            (self.two, self.rows, r.at[a, self.two], cross),
        )[i]
        return self.copy(a, block, rows, i, sem, to)

    def twin(self, a, block):
        ref = self.bufs[a].at[block, self.rows]
        return pltpu.make_async_remote_copy(
            src_ref=ref, dst_ref=ref, send_sem=self.dssem.at[a, block], recv_sem=self.dsem.at[a, block],
            device_id=self.sibling, device_id_type=MESH)

    def pass_on(self, a, block):
        if self.halves:
            self.twin(a, block).start()

    def start(self, a):
        for i in range(3):
            self.send(a, i).start()

    def phase1(self):
        for a in range(len(self.bufs)):
            self.got(a, self.down, self.rows, self.rsem.at[a, self.down])
            self.send(a, 3).start()
            self.got(a, self.up, self.rows, self.rsem.at[a, self.up])
            self.send(a, 4).start()
            self.got(a, self.cross, self.rows, self.rsem.at[a, self.cross])
            self.send(a, 5).start()
            self.send(a, 6).start()
            for b in (self.down, self.up, self.cross):
                self.pass_on(a, b)

    def phase2(self):
        for a in range(len(self.bufs)):
            self.got(a, self.two, self.low, self.psem.at[a, 0])
            self.got(a, self.two, self.high, self.psem.at[a, 1])
            self.send(a, 7).start()
            self.pass_on(a, self.two)

    def phase3(self):
        for a in range(len(self.bufs)):
            for b in (self.cdown, self.cup):
                self.got(a, b, self.rows, self.rsem.at[a, b])
                self.pass_on(a, b)

    def phase4(self):
        for a in range(len(self.bufs)):
            self.got(a, self.ctwo, self.rows, self.rsem.at[a, self.ctwo])
            self.pass_on(a, self.ctwo)

    def phases(self, k):
        seg = self.seg
        for phase, times in ((self.phase1, (1, 0, 0, 0, 0, 0, 0, 0)), (self.phase2, (2, 3, 0, 1, 1, 0, 0, 0)),
                             (self.phase3, (5, 4, 4, 4, 1, 0, 0, 0)), (self.phase4, (6, 7, 4, 5, 2, 3, 0, 1))):
            pl.when(table(seg, times) == k)(phase)

    def need(self, a, k):
        if self.halves:
            @pl.when(k != self.seg)
            def _():
                n = NB // 2
                e = lax.axis_index("energy")
                other = pl.ds(pl.multiple_of((1 - e % 2) * n, 8), n)
                self.got(a, k, other, self.dsem.at[a, k])

    def finish(self):
        for a in range(len(self.bufs)):
            for i in range(8):
                self.send(a, i).wait_send()
            if self.halves:
                for b in (self.down, self.up, self.cross, self.two, self.cdown, self.cup, self.ctwo):
                    self.twin(a, b).wait_send()


def entry_barrier(with_sibling):
    e = lax.axis_index("energy")
    seg = lax.axis_index("seg")
    pair, y = seg // 4, seg % 4
    to = [{"seg": pair * 4 + (y + 1) % 4}, {"seg": pair * 4 + (y + 3) % 4}, {"seg": (1 - pair) * 4 + y}]
    if with_sibling:
        to.append({"energy": e + 1 - 2 * (e % 2)})
    barrier = pltpu.get_barrier_semaphore()
    for d in to:
        pl.semaphore_signal(barrier, inc=1, device_id=d, device_id_type=MESH)
    pl.semaphore_wait(barrier, len(to))


def identity():
    row = lax.broadcasted_iota(jnp.int32, (NB, NB), 0)
    col = lax.broadcasted_iota(jnp.int32, (NB, NB), 1)
    return (row == col).astype(f32)


def invert_into(L, s, x, e_s, r_s, b_s):
    eye = identity()
    diag = x * eye
    d_row = 1.0 / jnp.sum(diag, axis=0, keepdims=True)
    d_col = 1.0 / jnp.sum(diag, axis=1, keepdims=True)
    e = eye - x * d_row
    put(e_s, e)
    b = eye + e
    r = mm(rd(e_s), rd(e_s))
    put(r_s.at[0], r)
    put(b_s, b)
    b = b + mm(rd(r_s.at[0]), rd(b_s))
    r = mm(rd(r_s.at[0]), rd(r_s.at[0]))
    put(r_s.at[1], r)
    put(b_s, b)
    b = b + mm(rd(r_s.at[1]), rd(b_s))
    r = mm(rd(r_s.at[1]), rd(r_s.at[1]))
    put(r_s.at[0], r)
    put(b_s, b)
    b = b + mm(rd(r_s.at[0]), rd(b_s))
    L[s] = b * d_col


def sweep(g, base_at, prepare, C, L, P, Q, e_s, r_s, b_s, out):
    seg = lax.axis_index("seg")
    g.phases(0)
    prepare(0)
    x0 = base_at(0) - 0.25 * mm(rd(C.at[0]), rd(C.at[0]), dott)
    invert_into(L, 0, x0, e_s, r_s, b_s)

    def forward(k, carry):
        g.phases(k)
        prepare(k)
        c = rd(C.at[k])
        put(b_s, L[k - 1])
        put(Q.at[k], mm(c, rd(b_s)))
        x = base_at(k) - mm(rd(Q.at[k]), c, dott)
        put(P.at[k], mm(rd(b_s), c, dott))
        invert_into(L, k, x, e_s, r_s, b_s)
        return carry

    lax.fori_loop(1, SEGS, forward, 0)
    out[...] = L[SEGS - 1]

    def backward(i, carry):
        t = SEGS - 1 - i
        put(b_s, out[...])
        put(e_s, mm(rd(P.at[t]), rd(b_s)))
        out[...] = L[t - 1] + mm(rd(e_s), rd(Q.at[t]))
        return carry

    lax.fori_loop(0, SEGS - 1 - seg, backward, 0)


def first_kernel(lev_ref, m_ref, c_ref, o_ref, call_ref, mall_ref,
                 cb, mb, C, L, P, Q, e_s, r_s, b_s, rsem, psem, ssem, dsem, dssem, lsem):
    seg = lax.axis_index("seg")
    own = [pltpu.make_async_copy(c_ref.at[0], cb.at[seg], lsem.at[0]),
           pltpu.make_async_copy(m_ref.at[0], mb.at[seg], lsem.at[1])]
    for c in own:
        c.start()
    entry_barrier(True)
    g = Gather((cb, mb), rsem, psem, ssem, dsem, dssem, True)
    for a, c in enumerate(own):
        c.wait()
        g.start(a)

    def prepare(k):
        g.need(0, k)
        g.need(1, k)
        put(C.at[k], cb[k])

    def base_at(k):
        return mb[k] + lev_ref[0] * identity()

    sweep(g, base_at, prepare, C, L, P, Q, e_s, r_s, b_s, o_ref)
    out = [pltpu.make_async_copy(cb, call_ref, lsem.at[0]), pltpu.make_async_copy(mb, mall_ref, lsem.at[1])]
    for c in out:
        c.start()
    g.finish()
    for c in out:
        c.wait()


def second_kernel(lev_ref, phi_ref, comb_ref, m_ref, c_ref, o_ref, se_ref,
                  sb, mb, cb, C, L, P, Q, e_s, r_s, b_s, rsem, psem, ssem, lsem):
    seg = lax.axis_index("seg")
    local = [pltpu.make_async_copy(c_ref, cb, lsem.at[0]), pltpu.make_async_copy(m_ref, mb, lsem.at[1])]
    for c in local:
        c.start()
    phi = split(phi_ref[0])
    half = mm(phi, split(comb_ref[...]))
    sb[seg] = mm(split(half), phi, dott)
    entry_barrier(False)
    g = Gather((sb,), rsem, psem, ssem, None, None, False)
    se_ref[...] = sb[seg]
    g.start(0)
    for c in local:
        c.wait()

    def prepare(k):
        put(C.at[k], cb[k])

    def base_at(k):
        return mb[k] + lev_ref[0] * identity() + sb[k]

    sweep(g, base_at, prepare, C, L, P, Q, e_s, r_s, b_s, o_ref)
    g.finish()


def block(n=None):
    return pltpu.VMEM((NB, NB) if n is None else (n, NB, NB), f32)


def pairs(n=None):
    return pltpu.VMEM((2, NB, NB) if n is None else (n, 2, NB, NB), bf16)


WORK = [pairs(8), block(8), pairs(8), pairs(8), pairs(), pairs(2), pairs()]
DMA = pltpu.SemaphoreType.DMA
VM = pl.BlockSpec(memory_space=pltpu.VMEM)
SM = pl.BlockSpec(memory_space=pltpu.SMEM)
ANY = pl.BlockSpec(memory_space=pl.ANY)
ONE = jax.ShapeDtypeStruct((NB, NB), f32)
ALL = jax.ShapeDtypeStruct((SEGS, NB, NB), f32)


def first_round(levels, onsite, coupling):
    return pl.pallas_call(
        first_kernel, out_shape=(ONE, ALL, ALL),
        in_specs=[SM, ANY, ANY], out_specs=(VM, ANY, ANY),
        scratch_shapes=[block(8), block(8)] + WORK + [DMA((2, 8)), DMA((2, 2)), DMA((2, 8)), DMA((2, 8)), DMA((2, 8)), DMA((2,))],
        compiler_params=pltpu.CompilerParams(vmem_limit_bytes=60 << 20, collective_id=0, has_side_effects=True),
        name="first_round",
    )(levels, onsite, coupling)


def second_round(levels, phonon, combined, onsite_all, coupling_all):
    return pl.pallas_call(
        second_kernel, out_shape=(ONE, ONE),
        in_specs=[SM, VM, VM, ANY, ANY], out_specs=(VM, VM),
        scratch_shapes=[block(8), block(8), block(8)] + WORK + [DMA((1, 8)), DMA((1, 2)), DMA((1, 8)), DMA((2,))],
        compiler_params=pltpu.CompilerParams(vmem_limit_bytes=60 << 20, collective_id=1, has_side_effects=True),
        name="second_round",
    )(levels, phonon, combined, onsite_all, coupling_all)


def energy_sum(green, offsets):
    count = lax.axis_size("energy")
    rows = NB // count
    pieces = lax.all_to_all(green.reshape(count, rows, NB), "energy", 0, 0, tiled=True)
    reach = count // 2
    padded = jnp.pad(pieces, ((reach, reach), (0, 0), (0, 0)))

    def moved(amount):
        return lax.dynamic_slice_in_dim(padded, reach - amount, count, 0)

    combined = moved(offsets[0]) + moved(offsets[1]) + moved(-offsets[0]) + moved(-offsets[1])
    return lax.all_to_all(combined, "energy", 0, 0, tiled=True).reshape(NB, NB)


def shards(onsite, coupling, phonon, levels, offsets):
    green, coupling_all, onsite_all = first_round(levels, onsite, coupling)
    combined = energy_sum(green, offsets)
    green, self_energy = second_round(levels, phonon, combined, onsite_all, coupling_all)
    return green[None, None], self_energy[None, None]


def solution(mesh):
    spec = jax.sharding.PartitionSpec
    block_in = spec("seg", None, None)
    block_out = spec("energy", "seg", None, None)
    return jax.shard_map(shards, mesh=mesh, in_specs=(block_in, block_in, block_in, spec("energy"), spec()),
                         out_specs=(block_out, block_out), check_vma=False)
```

```python
import functools
import jax
import jax.numpy as jnp
from jax import lax
from jax.experimental import pallas as pl
from jax.experimental.pallas import tpu as pltpu

NB = 384
SEGS = 8
ENERGIES = 32
CHIPS = ENERGIES // 2
SLAB = NB // CHIPS
PAD = 15
f32 = jnp.float32
bf16 = jnp.bfloat16
MESH = pl.DeviceIdType.MESH


def split(x):
    hi = x.astype(bf16)
    lo = (x - hi.astype(f32)).astype(bf16)
    return hi, lo


def put(ref, x):
    hi, lo = split(x)
    ref[0] = hi
    ref[1] = lo


def rd(ref):
    return ref[0], ref[1]


def dot(a, b):
    return lax.dot_general(a, b, (((1,), (0,)), ((), ())), preferred_element_type=f32)


def dott(a, b):
    return lax.dot_general(a, b, (((1,), (1,)), ((), ())), preferred_element_type=f32)


def mm(a, b, d=dot):
    ah, al = a
    bh, bl = b
    return d(ah, bh) + (d(ah, bl) + d(al, bh))


def table(seg, values):
    out = jnp.int32(values[-1])
    for i, v in enumerate(values[:-1]):
        out = jnp.where(seg == i, jnp.int32(v), out)
    return out


class Gather:
    def __init__(self, bufs, rsem, psem, ssem, dsem, dssem, halves):
        self.bufs, self.rsem, self.psem, self.ssem, self.dsem, self.dssem = bufs, rsem, psem, ssem, dsem, dssem
        e = lax.axis_index("energy")
        self.seg = lax.axis_index("seg")
        core = e % 2
        self.sibling = {"energy": e + 1 - 2 * core}
        pair, y = self.seg // 4, self.seg % 4
        at = lambda p, dy: p * 4 + (y + dy) % 4
        self.up, self.down, self.two = at(pair, 1), at(pair, 3), at(pair, 2)
        self.cross, self.cup, self.cdown, self.ctwo = at(1 - pair, 0), at(1 - pair, 1), at(1 - pair, 3), at(1 - pair, 2)
        self.halves = halves
        n = NB // 2 if halves else NB
        base = core * n if halves else 0
        self.rows = pl.ds(pl.multiple_of(base, 8), n)
        self.low = pl.ds(pl.multiple_of(base, 8), n // 2)
        self.high = pl.ds(pl.multiple_of(base + n // 2, 8), n // 2)

    def copy(self, a, block, rows, s, sem, to):
        ref = self.bufs[a].at[block, rows]
        return pltpu.make_async_remote_copy(
            src_ref=ref, dst_ref=ref, send_sem=self.ssem.at[a, s], recv_sem=sem,
            device_id=to, device_id_type=MESH)

    def got(self, a, block, rows, sem):
        self.copy(a, block, rows, 0, sem, {"seg": self.up}).wait_recv()

    def send(self, a, i):
        r, p = self.rsem, self.psem
        up, down, cross = {"seg": self.up}, {"seg": self.down}, {"seg": self.cross}
        block, rows, sem, to = (
            (self.seg, self.rows, r.at[a, self.seg], up),
            (self.seg, self.rows, r.at[a, self.seg], down),
            (self.seg, self.rows, r.at[a, self.seg], cross),
            (self.down, self.low, p.at[a, 0], up),
            (self.up, self.high, p.at[a, 1], down),
            (self.cross, self.rows, r.at[a, self.cross], up),
            (self.cross, self.rows, r.at[a, self.cross], down),
            (self.two, self.rows, r.at[a, self.two], cross),
        )[i]
        return self.copy(a, block, rows, i, sem, to)

    def twin(self, a, block):
        ref = self.bufs[a].at[block, self.rows]
        return pltpu.make_async_remote_copy(
            src_ref=ref, dst_ref=ref, send_sem=self.dssem.at[a, block], recv_sem=self.dsem.at[a, block],
            device_id=self.sibling, device_id_type=MESH)

    def pass_on(self, a, block):
        if self.halves:
            self.twin(a, block).start()

    def start(self, a):
        for i in range(3):
            self.send(a, i).start()

    def phase1(self):
        for a in range(len(self.bufs)):
            self.got(a, self.down, self.rows, self.rsem.at[a, self.down])
            self.send(a, 3).start()
            self.got(a, self.up, self.rows, self.rsem.at[a, self.up])
            self.send(a, 4).start()
            self.got(a, self.cross, self.rows, self.rsem.at[a, self.cross])
            self.send(a, 5).start()
            self.send(a, 6).start()
            for b in (self.down, self.up, self.cross):
                self.pass_on(a, b)

    def phase2(self):
        for a in range(len(self.bufs)):
            self.got(a, self.two, self.low, self.psem.at[a, 0])
            self.got(a, self.two, self.high, self.psem.at[a, 1])
            self.send(a, 7).start()
            self.pass_on(a, self.two)

    def phase3(self):
        for a in range(len(self.bufs)):
            for b in (self.cdown, self.cup):
                self.got(a, b, self.rows, self.rsem.at[a, b])
                self.pass_on(a, b)

    def phase4(self):
        for a in range(len(self.bufs)):
            self.got(a, self.ctwo, self.rows, self.rsem.at[a, self.ctwo])
            self.pass_on(a, self.ctwo)

    def phases(self, k):
        seg = self.seg
        for phase, times in ((self.phase1, (1, 0, 0, 0, 0, 0, 0, 0)), (self.phase2, (2, 3, 0, 1, 1, 0, 0, 0)),
                             (self.phase3, (5, 4, 4, 4, 1, 0, 0, 0)), (self.phase4, (6, 7, 4, 5, 2, 3, 0, 1))):
            pl.when(table(seg, times) == k)(phase)

    def need(self, a, k):
        if self.halves:
            @pl.when(k != self.seg)
            def _():
                n = NB // 2
                e = lax.axis_index("energy")
                other = pl.ds(pl.multiple_of((1 - e % 2) * n, 8), n)
                self.got(a, k, other, self.dsem.at[a, k])

    def finish(self):
        for a in range(len(self.bufs)):
            for i in range(8):
                self.send(a, i).wait_send()
            if self.halves:
                for b in (self.down, self.up, self.cross, self.two, self.cdown, self.cup, self.ctwo):
                    self.twin(a, b).wait_send()


def entry_barrier():
    e = lax.axis_index("energy")
    seg = lax.axis_index("seg")
    core = e % 2
    pair, y = seg // 4, seg % 4
    barrier = pltpu.get_barrier_semaphore()

    def hello(to):
        pl.semaphore_signal(barrier, inc=1, device_id=to, device_id_type=MESH)

    for other in (pair * 4 + (y + 1) % 4, pair * 4 + (y + 3) % 4, (1 - pair) * 4 + y):
        hello({"seg": other})
    for d in range(1, 32):
        other = (e + d) % 32

        @pl.when((core == 1) | (other % 2 == 1))
        def _():
            hello({"energy": other})

    pl.semaphore_wait(barrier, 3 + 16 + 15 * core)


def identity():
    row = lax.broadcasted_iota(jnp.int32, (NB, NB), 0)
    col = lax.broadcasted_iota(jnp.int32, (NB, NB), 1)
    return (row == col).astype(f32)


def invert_into(L, s, x, e_s, r_s, b_s):
    eye = identity()
    diag = x * eye
    d_row = 1.0 / jnp.sum(diag, axis=0, keepdims=True)
    d_col = 1.0 / jnp.sum(diag, axis=1, keepdims=True)
    e = eye - x * d_row
    put(e_s, e)
    b = eye + e
    r = mm(rd(e_s), rd(e_s))
    put(r_s.at[0], r)
    put(b_s, b)
    b = b + mm(rd(r_s.at[0]), rd(b_s))
    r = mm(rd(r_s.at[0]), rd(r_s.at[0]))
    put(r_s.at[1], r)
    put(b_s, b)
    b = b + mm(rd(r_s.at[1]), rd(b_s))
    r = mm(rd(r_s.at[1]), rd(r_s.at[1]))
    put(r_s.at[0], r)
    put(b_s, b)
    b = b + mm(rd(r_s.at[0]), rd(b_s))
    L[s] = b * d_col


def sweep(g, base_at, prepare, C, L, P, Q, e_s, r_s, b_s, out):
    seg = lax.axis_index("seg")
    g.phases(0)
    prepare(0)
    x0 = base_at(0) - 0.25 * mm(rd(C.at[0]), rd(C.at[0]), dott)
    invert_into(L, 0, x0, e_s, r_s, b_s)

    def forward(k, carry):
        g.phases(k)
        prepare(k)
        c = rd(C.at[k])
        put(b_s, L[k - 1])
        put(Q.at[k], mm(c, rd(b_s)))
        x = base_at(k) - mm(rd(Q.at[k]), c, dott)
        put(P.at[k], mm(rd(b_s), c, dott))
        invert_into(L, k, x, e_s, r_s, b_s)
        return carry

    lax.fori_loop(1, SEGS, forward, 0)
    out[...] = L[SEGS - 1]

    def backward(i, carry):
        t = SEGS - 1 - i
        put(b_s, out[...])
        put(e_s, mm(rd(P.at[t]), rd(b_s)))
        out[...] = L[t - 1] + mm(rd(e_s), rd(Q.at[t]))
        return carry

    lax.fori_loop(0, SEGS - 1 - seg, backward, 0)


def exchange(green, off_ref, got, slabs, combined, out_ssem, out_rsem, back_ssem, back_rsem):
    e = lax.axis_index("energy")
    core, chip = e % 2, e // 2
    adder = core == 1

    def slab_rows(j):
        return pl.ds(pl.multiple_of(j * SLAB, 8), SLAB)

    def out_copy(j, source):
        return pltpu.make_async_remote_copy(
            src_ref=green.at[slab_rows(j)], dst_ref=got.at[PAD + source], send_sem=out_ssem.at[j], recv_sem=out_rsem.at[source],
            device_id={"energy": 2 * j + 1}, device_id_type=MESH)

    def back_copy(energy, j):
        return pltpu.make_async_remote_copy(
            src_ref=slabs.at[energy], dst_ref=combined.at[slab_rows(j)], send_sem=back_ssem.at[energy], recv_sem=back_rsem.at[j],
            device_id={"energy": energy}, device_id_type=MESH)

    def send_out(d, carry):
        j = (chip + d) % CHIPS

        @pl.when(e != 2 * j + 1)
        def _():
            out_copy(j, e).start()
        return carry

    lax.fori_loop(0, CHIPS, send_out, 0)

    @pl.when(adder)
    def _():
        got[PAD + e] = green[slab_rows(chip)]
        edge = jnp.zeros((SLAB, NB), f32)
        for i in range(PAD):
            got[i] = edge
            got[PAD + ENERGIES + i] = edge

        def receive(d, carry):
            source = (e + d) % ENERGIES
            out_copy(chip, source).wait_recv()
            return carry

        lax.fori_loop(1, ENERGIES, receive, 0)
        o1, o2 = off_ref[0], off_ref[1]

        def add(i, carry):
            p = PAD + i
            slabs[i] = got[p - o1] + got[p - o2] + got[p + o1] + got[p + o2]
            return carry

        lax.fori_loop(0, ENERGIES, add, 0)
        combined[slab_rows(chip)] = slabs[e]

        def send_back(d, carry):
            back_copy((e + d) % ENERGIES, chip).start()
            return carry

        lax.fori_loop(1, ENERGIES, send_back, 0)

    def receive_back(j, carry):
        @pl.when(e != 2 * j + 1)
        def _():
            back_copy(e, j).wait_recv()
        return carry

    lax.fori_loop(0, CHIPS, receive_back, 0)

    def finish():
        def sent_out(j, carry):
            @pl.when(e != 2 * j + 1)
            def _():
                out_copy(j, e).wait_send()
            return carry

        lax.fori_loop(0, CHIPS, sent_out, 0)

        @pl.when(adder)
        def _():
            def sent_back(d, carry):
                back_copy((e + d) % ENERGIES, chip).wait_send()
                return carry

            lax.fori_loop(1, ENERGIES, sent_back, 0)

    return finish


def whole_kernel(lev_ref, off_ref, phi_ref, m_ref, c_ref, o_ref, se_ref,
                 cb, mb, sb, C, L, P, Q, e_s, r_s, b_s, green, got, slabs, combined,
                 rsem, psem, ssem, dsem, dssem, rsem2, psem2, ssem2, out_ssem, out_rsem, back_ssem, back_rsem, lsem):
    seg = lax.axis_index("seg")
    own = [pltpu.make_async_copy(c_ref.at[0], cb.at[seg], lsem.at[0]),
           pltpu.make_async_copy(m_ref.at[0], mb.at[seg], lsem.at[1])]
    for c in own:
        c.start()
    entry_barrier()
    g = Gather((cb, mb), rsem, psem, ssem, dsem, dssem, True)
    for a, c in enumerate(own):
        c.wait()
        g.start(a)

    def prepare(k):
        g.need(0, k)
        g.need(1, k)
        put(C.at[k], cb[k])

    def base_at(k):
        return mb[k] + lev_ref[0] * identity()

    sweep(g, base_at, prepare, C, L, P, Q, e_s, r_s, b_s, green)
    finish = exchange(green, off_ref, got, slabs, combined, out_ssem, out_rsem, back_ssem, back_rsem)
    phi = split(phi_ref[0])
    half = mm(phi, split(combined[...]))
    sb[seg] = mm(split(half), phi, dott)
    g2 = Gather((sb,), rsem2, psem2, ssem2, None, None, False)
    g2.start(0)
    se_ref[...] = sb[seg]
    sweep(g2, lambda k: base_at(k) + sb[k], lambda k: None, C, L, P, Q, e_s, r_s, b_s, o_ref)
    finish()
    g.finish()
    g2.finish()


def block(n=None):
    return pltpu.VMEM((NB, NB) if n is None else (n, NB, NB), f32)


def pairs(n=None):
    return pltpu.VMEM((2, NB, NB) if n is None else (n, 2, NB, NB), bf16)


WORK = [pairs(8), block(8), pairs(8), pairs(8), pairs(), pairs(2), pairs()]
DMA = pltpu.SemaphoreType.DMA
VM = pl.BlockSpec(memory_space=pltpu.VMEM)
SM = pl.BlockSpec(memory_space=pltpu.SMEM)
ANY = pl.BlockSpec(memory_space=pl.ANY)
ONE = jax.ShapeDtypeStruct((NB, NB), f32)
ALL = jax.ShapeDtypeStruct((SEGS, NB, NB), f32)


def whole(levels, offsets, phonon, onsite, coupling):
    return pl.pallas_call(
        whole_kernel, out_shape=(ONE, ONE),
        in_specs=[SM, SM, VM, ANY, ANY], out_specs=(VM, VM),
        scratch_shapes=[block(8), block(8), block(8)] + WORK + [
            block(), pltpu.VMEM((ENERGIES + 2 * PAD, SLAB, NB), f32), pltpu.VMEM((ENERGIES, SLAB, NB), f32), block(),
            DMA((2, 8)), DMA((2, 2)), DMA((2, 8)), DMA((2, 8)), DMA((2, 8)),
            DMA((1, 8)), DMA((1, 2)), DMA((1, 8)),
            DMA((CHIPS,)), DMA((ENERGIES,)), DMA((ENERGIES,)), DMA((CHIPS,)), DMA((2,))],
        compiler_params=pltpu.CompilerParams(vmem_limit_bytes=62 << 20, collective_id=0, has_side_effects=True),
        name="born",
    )(levels, offsets, phonon, onsite, coupling)


def shards(onsite, coupling, phonon, levels, offsets):
    green, self_energy = whole(levels, offsets, phonon, onsite, coupling)
    return green[None, None], self_energy[None, None]


def solution(mesh):
    spec = jax.sharding.PartitionSpec
    block_in = spec("seg", None, None)
    block_out = spec("energy", "seg", None, None)
    return jax.shard_map(shards, mesh=mesh, in_specs=(block_in, block_in, block_in, spec("energy"), spec()),
                         out_specs=(block_out, block_out), check_vma=False)
```

```python
import functools
import jax
import jax.numpy as jnp
from jax import lax
from jax.experimental import pallas as pl
from jax.experimental.pallas import tpu as pltpu

NB = 384
SEGS = 8
ENERGIES = 32
CHIPS = ENERGIES // 2
SLAB = NB // CHIPS
PAD = 15
HALVES = 2
CUTS = 3
f32 = jnp.float32
bf16 = jnp.bfloat16
MESH = pl.DeviceIdType.MESH


def split(x):
    hi = x.astype(bf16)
    lo = (x - hi.astype(f32)).astype(bf16)
    return hi, lo


def put_left(ref, x):
    hi, lo = split(x)
    ref[:, 0:256] = hi[:, 0:256]
    ref[:, 256:512] = lo[:, 0:256]
    ref[:, 512:640] = hi[:, 256:384]
    ref[:, 640:768] = lo[:, 256:384]


def put_right(ref, x):
    hi, lo = split(x)
    ref[0:256, 0:384] = hi[0:256]
    ref[256:512, 0:384] = hi[0:256]
    ref[0:256, 384:768] = lo[0:256]
    ref[512:640, 0:384] = hi[256:384]
    ref[640:768, 0:384] = hi[256:384]
    ref[512:640, 384:768] = lo[256:384]


def clear_right(ref):
    ref[256:512, 384:768] = jnp.zeros((256, 384), bf16)
    ref[640:768, 384:768] = jnp.zeros((128, 384), bf16)


def dot(a, b):
    return lax.dot_general(a, b, (((1,), (0,)), ((), ())), preferred_element_type=f32)


def mm(l, r):
    out = []
    for h in range(HALVES):
        n = NB // HALVES
        rows = slice(h * n, h * n + n)
        a = dot(l[rows, :], r[:, 0:512])
        b = dot(l[rows, 0:256], r[0:256, 512:768]) + dot(l[rows, 512:768], r[512:768, 512:768])
        out.append(jnp.concatenate([a[:, 0:128] + a[:, 384:512], a[:, 128:384] + b], axis=1))
    return jnp.concatenate(out, axis=0)


def table(seg, values):
    out = jnp.int32(values[-1])
    for i, v in enumerate(values[:-1]):
        out = jnp.where(seg == i, jnp.int32(v), out)
    return out


class Gather:
    def __init__(self, parts, rsem, psem, ssem, dsem, dssem):
        self.parts, self.rsem, self.psem, self.ssem, self.dsem, self.dssem = parts, rsem, psem, ssem, dsem, dssem
        self.each = range(len(parts))
        self.twins = dsem is not None
        e = lax.axis_index("energy")
        self.seg = lax.axis_index("seg")
        self.sibling = {"energy": e + 1 - 2 * (e % 2)}
        self.pair, self.y = self.seg // 4, self.seg % 4
        at = lambda p, dy: p * 4 + (self.y + dy) % 4
        self.up, self.down, self.two = at(self.pair, 1), at(self.pair, 3), at(self.pair, 2)
        other = 1 - self.pair
        self.cross, self.cup, self.cdown, self.ctwo = at(other, 0), at(other, 1), at(other, 3), at(other, 2)

    def view(self, a, block, part=None):
        ref, base, n = self.parts[a]
        if part is not None:
            n = n // 2
            base = base + part * n
        return ref.at[block, pl.ds(pl.multiple_of(base, 8), n)]

    def copy(self, a, block, part, s, sem, to):
        ref = self.view(a, block, part)
        return pltpu.make_async_remote_copy(
            src_ref=ref, dst_ref=ref, send_sem=self.ssem.at[a, s], recv_sem=sem,
            device_id=to, device_id_type=MESH)

    def got(self, a, block, part=None):
        sem = self.rsem.at[a, block] if part is None else self.psem.at[a, part]
        self.copy(a, block, part, 0, sem, {"seg": self.up}).wait_recv()

    def send(self, a, i):
        r, p = self.rsem, self.psem
        up, down, cross = {"seg": self.up}, {"seg": self.down}, {"seg": self.cross}
        block, part, sem, to = (
            (self.seg, None, r.at[a, self.seg], up),
            (self.seg, None, r.at[a, self.seg], down),
            (self.seg, None, r.at[a, self.seg], cross),
            (self.down, 0, p.at[a, 0], up),
            (self.up, 1, p.at[a, 1], down),
            (self.cross, None, r.at[a, self.cross], up),
            (self.cross, None, r.at[a, self.cross], down),
            (self.two, None, r.at[a, self.two], cross),
        )[i]
        return self.copy(a, block, part, i, sem, to)

    def twin(self, a, block):
        ref = self.view(a, block)
        return pltpu.make_async_remote_copy(
            src_ref=ref, dst_ref=ref, send_sem=self.dssem.at[a, block], recv_sem=self.dsem.at[a, block],
            device_id=self.sibling, device_id_type=MESH)

    def pass_on(self, a, block):
        if self.twins:
            self.twin(a, block).start()

    def start(self, a):
        for i in range(3):
            self.send(a, i).start()

    def take(self, a, block, *sends):
        self.got(a, block)
        for i in sends:
            self.send(a, i).start()
        self.pass_on(a, block)

    def phase1(self):
        first = self.pair == 0

        @pl.when(first & (self.y == 1))
        def _():
            for a in self.each:
                self.take(a, self.up, 4)
            for a in self.each:
                self.take(a, self.cross, 6)
            for a in self.each:
                self.take(a, self.down, 3)
            for a in self.each:
                self.send(a, 5).start()

        @pl.when(first & (self.y == 3))
        def _():
            for a in self.each:
                self.take(a, self.down, 3)
            for a in self.each:
                self.take(a, self.cross, 5)
            for a in self.each:
                self.take(a, self.up, 4)
            for a in self.each:
                self.send(a, 6).start()

        @pl.when(jnp.logical_not(first & (self.y % 2 == 1)))
        def _():
            for a in self.each:
                self.take(a, self.down, 3)
                self.take(a, self.up, 4)
            for a in self.each:
                self.take(a, self.cross, 5, 6)

    def phase2(self):
        for a in self.each:
            self.got(a, self.two, 0)
            self.got(a, self.two, 1)
            self.send(a, 7).start()
            self.pass_on(a, self.two)

    def phase3(self):
        for a in self.each:
            for b in (self.cdown, self.cup):
                self.take(a, b)

    def phase4(self):
        for a in self.each:
            self.take(a, self.ctwo)

    def phases(self, k):
        for phase, times in ((self.phase1, (1, 0, 0, 0, 0, 0, 0, 0)), (self.phase2, (2, 3, 0, 1, 1, 0, 0, 0)),
                             (self.phase3, (5, 4, 4, 4, 1, 0, 0, 0)), (self.phase4, (6, 7, 4, 5, 2, 3, 0, 1))):
            pl.when(table(self.seg, times) == k)(phase)

    def need(self, a, k):
        @pl.when(k != self.seg)
        def _():
            ref, base, n = self.parts[a]
            other = ref.at[k, pl.ds(pl.multiple_of(n - base, 8), n)]
            pltpu.make_async_remote_copy(
                src_ref=other, dst_ref=other, send_sem=self.dssem.at[a, k], recv_sem=self.dsem.at[a, k],
                device_id=self.sibling, device_id_type=MESH).wait_recv()

    def finish(self):
        for a in self.each:
            for i in range(8):
                self.send(a, i).wait_send()
            if self.twins:
                for b in (self.down, self.up, self.cross, self.two, self.cdown, self.cup, self.ctwo):
                    self.twin(a, b).wait_send()


def entry_barrier():
    e = lax.axis_index("energy")
    seg = lax.axis_index("seg")
    core = e % 2
    pair, y = seg // 4, seg % 4
    barrier = pltpu.get_barrier_semaphore()

    def hello(to):
        pl.semaphore_signal(barrier, inc=1, device_id=to, device_id_type=MESH)

    for other in (pair * 4 + (y + 1) % 4, pair * 4 + (y + 3) % 4, (1 - pair) * 4 + y):
        hello({"seg": other})
    for d in range(1, 32):
        other = (e + d) % 32

        @pl.when((core == 1) | (other % 2 == 1))
        def _():
            hello({"energy": other})

    pl.semaphore_wait(barrier, 3 + 16 + 15 * core)


def identity():
    row = lax.broadcasted_iota(jnp.int32, (NB, NB), 0)
    col = lax.broadcasted_iota(jnp.int32, (NB, NB), 1)
    return (row == col).astype(f32)


def invert_into(L, s, x, el, rl, er, rr, br, fill=None):
    eye = identity()
    diag = x * eye
    d_col = 1.0 / jnp.sum(diag, axis=1, keepdims=True)
    d_row = 1.0 / jnp.sum(diag, axis=0, keepdims=True)
    e = eye - x * d_col
    put_left(el, e)
    put_right(er, e)
    if fill is not None:
        fill()
    r = mm(el, er)
    put_left(rl, r)
    put_right(rr, r)
    b = eye + e
    put_right(br, b)
    r = mm(rl, rr)
    b = b + mm(rl, br)
    put_left(el, r)
    put_right(er, r)
    put_right(br, b)
    r = mm(el, er)
    b = b + mm(el, br)
    put_left(rl, r)
    put_right(br, b)
    b = b + mm(rl, br)
    L[s] = b * d_row


def sweep(g, base_at, prepare, first, w, out):
    L, P, Q, C, CT, el, rl, er, rr, br, ql, ll = w
    seg = lax.axis_index("seg")
    g.phases(0)
    prepare(0)
    invert_into(L, 0, first(), el, rl, er, rr, br)

    def forward(k, carry):
        g.phases(k)
        prepare(k)
        left = L[k - 1]
        put_right(br, left)
        put_left(ll, left)
        q = mm(C.at[k], br)
        put_left(ql, q)
        put_right(Q.at[k], q)
        x = base_at(k) - mm(ql, CT.at[k])

        def fill():
            put_left(P.at[k], mm(ll, CT.at[k]))

        invert_into(L, k, x, el, rl, er, rr, br, fill)
        return carry

    lax.fori_loop(1, SEGS, forward, 0)
    out[...] = L[SEGS - 1]

    def backward(i, carry):
        t = SEGS - 1 - i
        put_right(br, out[...])
        put_left(el, mm(P.at[t], br))
        out[...] = L[t - 1] + mm(el, Q.at[t])
        return carry

    lax.fori_loop(0, SEGS - 1 - seg, backward, 0)


def exchange(green, off_ref, got, slabs, combined, out_ssem, out_rsem, back_ssem, back_rsem, meanwhile):
    e = lax.axis_index("energy")
    core, chip = e % 2, e // 2
    adder = core == 1

    def slab_rows(j):
        return pl.ds(pl.multiple_of(j * SLAB, 8), SLAB)

    def out_copy(j, source):
        return pltpu.make_async_remote_copy(
            src_ref=green.at[slab_rows(j)], dst_ref=got.at[PAD + source], send_sem=out_ssem.at[j], recv_sem=out_rsem.at[source],
            device_id={"energy": 2 * j + 1}, device_id_type=MESH)

    def back_copy(energy, j):
        return pltpu.make_async_remote_copy(
            src_ref=slabs.at[energy], dst_ref=combined.at[slab_rows(j)], send_sem=back_ssem.at[energy], recv_sem=back_rsem.at[j],
            device_id={"energy": energy}, device_id_type=MESH)

    def send_out(d, carry):
        j = (chip + d) % CHIPS

        @pl.when(e != 2 * j + 1)
        def _():
            out_copy(j, e).start()
        return carry

    lax.fori_loop(0, CHIPS, send_out, 0)
    meanwhile()

    @pl.when(adder)
    def _():
        got[PAD + e] = green[slab_rows(chip)]
        edge = jnp.zeros((SLAB, NB), f32)
        for i in range(PAD):
            got[i] = edge
            got[PAD + ENERGIES + i] = edge

        def receive(d, carry):
            source = (e + d) % ENERGIES
            out_copy(chip, source).wait_recv()
            return carry

        lax.fori_loop(1, ENERGIES, receive, 0)
        o1, o2 = off_ref[0], off_ref[1]

        def add(i, carry):
            p = PAD + i
            slabs[i] = got[p - o1] + got[p - o2] + got[p + o1] + got[p + o2]
            return carry

        lax.fori_loop(0, ENERGIES, add, 0)
        combined[slab_rows(chip)] = slabs[e]

        def send_back(d, carry):
            back_copy((e + d) % ENERGIES, chip).start()
            return carry

        lax.fori_loop(1, ENERGIES, send_back, 0)

    def receive_back(j, carry):
        @pl.when(e != 2 * j + 1)
        def _():
            back_copy(e, j).wait_recv()
        return carry

    lax.fori_loop(0, CHIPS, receive_back, 0)

    def finish():
        def sent_out(j, carry):
            @pl.when(e != 2 * j + 1)
            def _():
                out_copy(j, e).wait_send()
            return carry

        lax.fori_loop(0, CHIPS, sent_out, 0)

        @pl.when(adder)
        def _():
            def sent_back(d, carry):
                back_copy((e + d) % ENERGIES, chip).wait_send()
                return carry

            lax.fori_loop(1, ENERGIES, sent_back, 0)

    return finish


def whole_kernel(lev_ref, off_ref, phi_ref, m_ref, c_ref, o_ref, se_ref,
                 cb, mb, sb, L, P, Q, C, CT, el, rl, er, rr, br, ql, ll, base0, green, got, slabs, combined,
                 rsem, psem, ssem, dsem, dssem, rsem2, psem2, ssem2, out_ssem, out_rsem, back_ssem, back_rsem, lsem):
    seg = lax.axis_index("seg")
    own = [pltpu.make_async_copy(c_ref.at[0], cb.at[seg], lsem.at[0]),
           pltpu.make_async_copy(m_ref.at[0], mb.at[seg], lsem.at[1])]
    for c in own:
        c.start()
    entry_barrier()
    half = NB // 2
    mine = (lax.axis_index("energy") % 2) * half
    g = Gather(((cb, mine, half), (mb, mine, half)), rsem, psem, ssem, dsem, dssem)
    for a, c in enumerate(own):
        c.wait()
        g.start(a)
    for ref in (er, rr, br):
        clear_right(ref)
    w = (L, P, Q, C, CT, el, rl, er, rr, br, ql, ll)

    def prepare(k):
        clear_right(CT.at[k])
        clear_right(Q.at[k])
        g.need(0, k)
        g.need(1, k)
        c = cb[k]
        put_left(C.at[k], c)
        put_right(CT.at[k], c.T)

    def base_at(k):
        return mb[k] + lev_ref[0] * identity()

    def first():
        x = base_at(0) - 0.25 * mm(C.at[0], CT.at[0])
        base0[...] = x
        return x

    sweep(g, base_at, prepare, first, w, green)

    def meanwhile():
        phi = phi_ref[0]
        put_left(el, phi)
        put_right(rr, phi.T)

    finish = exchange(green, off_ref, got, slabs, combined, out_ssem, out_rsem, back_ssem, back_rsem, meanwhile)
    put_right(br, combined[...])
    put_left(ql, mm(el, br))
    sb[seg] = mm(ql, rr)
    third = NB // CUTS
    g2 = Gather([(sb, a * third, third) for a in range(CUTS)], rsem2, psem2, ssem2, None, None)
    for a in range(CUTS):
        g2.start(a)
    se_ref[...] = sb[seg]
    sweep(g2, lambda k: base_at(k) + sb[k], lambda k: None, lambda: base0[...] + sb[0], w, o_ref)
    finish()
    g.finish()
    g2.finish()


def block(n=None):
    return pltpu.VMEM((NB, NB) if n is None else (n, NB, NB), f32)


def left(*n):
    return pltpu.VMEM((*n, NB, 2 * NB), bf16)


def right(*n):
    return pltpu.VMEM((*n, 2 * NB, 2 * NB), bf16)


WORK = [block(8), left(8), right(8), left(8), right(8), left(), left(), right(), right(), right(), left(), left(), block()]
DMA = pltpu.SemaphoreType.DMA
VM = pl.BlockSpec(memory_space=pltpu.VMEM)
SM = pl.BlockSpec(memory_space=pltpu.SMEM)
ANY = pl.BlockSpec(memory_space=pl.ANY)
ONE = jax.ShapeDtypeStruct((NB, NB), f32)


def whole(levels, offsets, phonon, onsite, coupling):
    return pl.pallas_call(
        whole_kernel, out_shape=(ONE, ONE),
        in_specs=[SM, SM, VM, ANY, ANY], out_specs=(VM, VM),
        scratch_shapes=[block(8), block(8), block(8)] + WORK + [
            block(), pltpu.VMEM((ENERGIES + 2 * PAD, SLAB, NB), f32), pltpu.VMEM((ENERGIES, SLAB, NB), f32), block(),
            DMA((2, 8)), DMA((2, 2)), DMA((2, 8)), DMA((2, 8)), DMA((2, 8)),
            DMA((CUTS, 8)), DMA((CUTS, 2)), DMA((CUTS, 8)),
            DMA((CHIPS,)), DMA((ENERGIES,)), DMA((ENERGIES,)), DMA((CHIPS,)), DMA((2,))],
        compiler_params=pltpu.CompilerParams(vmem_limit_bytes=62 << 20, collective_id=0, has_side_effects=True),
        name="born",
    )(levels, offsets, phonon, onsite, coupling)


def shards(onsite, coupling, phonon, levels, offsets):
    green, self_energy = whole(levels, offsets, phonon, onsite, coupling)
    return green[None, None], self_energy[None, None]


def solution(mesh):
    spec = jax.sharding.PartitionSpec
    block_in = spec("seg", None, None)
    block_out = spec("energy", "seg", None, None)
    return jax.shard_map(shards, mesh=mesh, in_specs=(block_in, block_in, block_in, spec("energy"), spec()),
                         out_specs=(block_out, block_out), check_vma=False)
```

```python
import functools
import jax
import jax.numpy as jnp
from jax import lax
from jax.experimental import pallas as pl
from jax.experimental.pallas import tpu as pltpu

NB = 384
SEGS = 8
ENERGIES = 32
CHIPS = ENERGIES // 2
SLAB = NB // CHIPS
PAD = 15
HALVES = 2
CUTS = 6
PARTS = 3
f32 = jnp.float32
bf16 = jnp.bfloat16
MESH = pl.DeviceIdType.MESH


def split(x):
    hi = x.astype(bf16)
    lo = (x - hi.astype(f32)).astype(bf16)
    return hi, lo


def put_left(ref, x):
    hi, lo = split(x)
    ref[:, 0:256] = hi[:, 0:256]
    ref[:, 256:512] = lo[:, 0:256]
    ref[:, 512:640] = hi[:, 256:384]
    ref[:, 640:768] = lo[:, 256:384]


def put_right(ref, x):
    hi, lo = split(x)
    ref[0:256, 0:384] = hi[0:256]
    ref[256:512, 0:384] = hi[0:256]
    ref[0:256, 384:768] = lo[0:256]
    ref[512:640, 0:384] = hi[256:384]
    ref[640:768, 0:384] = hi[256:384]
    ref[512:640, 384:768] = lo[256:384]


def clear_right(ref):
    ref[256:512, 384:768] = jnp.zeros((256, 384), bf16)
    ref[640:768, 384:768] = jnp.zeros((128, 384), bf16)


def dot(a, b):
    return lax.dot_general(a, b, (((1,), (0,)), ((), ())), preferred_element_type=f32)


def mm(l, r):
    out = []
    for h in range(HALVES):
        n = NB // HALVES
        rows = slice(h * n, h * n + n)
        a = dot(l[rows, :], r[:, 0:512])
        b = dot(l[rows, 0:256], r[0:256, 512:768]) + dot(l[rows, 512:768], r[512:768, 512:768])
        out.append(jnp.concatenate([a[:, 0:128] + a[:, 384:512], a[:, 128:384] + b], axis=1))
    return jnp.concatenate(out, axis=0)


def table(seg, values):
    out = jnp.int32(values[-1])
    for i, v in enumerate(values[:-1]):
        out = jnp.where(seg == i, jnp.int32(v), out)
    return out


class Gather:
    def __init__(self, parts, rsem, psem, ssem, dsem, dssem):
        self.parts, self.rsem, self.psem, self.ssem, self.dsem, self.dssem = parts, rsem, psem, ssem, dsem, dssem
        self.each = range(len(parts))
        self.twins = dsem is not None
        e = lax.axis_index("energy")
        self.seg = lax.axis_index("seg")
        self.sibling = {"energy": e + 1 - 2 * (e % 2)}
        self.pair, self.y = self.seg // 4, self.seg % 4
        at = lambda p, dy: p * 4 + (self.y + dy) % 4
        self.up, self.down, self.two = at(self.pair, 1), at(self.pair, 3), at(self.pair, 2)
        other = 1 - self.pair
        self.cross, self.cup, self.cdown, self.ctwo = at(other, 0), at(other, 1), at(other, 3), at(other, 2)

    def view(self, a, block, part=None):
        ref, base, n = self.parts[a]
        if part is not None:
            n = n // 2
            base = base + part * n
        return ref.at[block, pl.ds(pl.multiple_of(base, 8), n)]

    def copy(self, a, block, part, s, sem, to):
        ref = self.view(a, block, part)
        return pltpu.make_async_remote_copy(
            src_ref=ref, dst_ref=ref, send_sem=self.ssem.at[a, s], recv_sem=sem,
            device_id=to, device_id_type=MESH)

    def got(self, a, block, part=None, base=0):
        sem = self.rsem.at[a, block] if part is None else self.psem.at[a, base + part]
        self.copy(a, block, part, 0, sem, {"seg": self.up}).wait_recv()

    def send(self, a, i):
        r, p = self.rsem, self.psem
        up, down, cross = {"seg": self.up}, {"seg": self.down}, {"seg": self.cross}
        block, part, sem, to = (
            (self.seg, None, r.at[a, self.seg], up),
            (self.seg, None, r.at[a, self.seg], down),
            (self.seg, None, r.at[a, self.seg], cross),
            (self.down, 0, p.at[a, 0], up),
            (self.up, 1, p.at[a, 1], down),
            (self.cross, None, r.at[a, self.cross], up),
            (self.cross, None, r.at[a, self.cross], down),
            (self.two, None, r.at[a, self.two], cross),
            (self.cdown, 0, p.at[a, 2], up),
            (self.cup, 1, p.at[a, 3], down),
        )[i]
        return self.copy(a, block, part, i, sem, to)

    def twin(self, a, block):
        ref = self.view(a, block)
        return pltpu.make_async_remote_copy(
            src_ref=ref, dst_ref=ref, send_sem=self.dssem.at[a, block], recv_sem=self.dsem.at[a, block],
            device_id=self.sibling, device_id_type=MESH)

    def pass_on(self, a, block):
        if self.twins:
            self.twin(a, block).start()

    def start(self, a):
        for i in range(3):
            self.send(a, i).start()

    def take(self, a, block, *sends):
        self.got(a, block)
        for i in sends:
            self.send(a, i).start()
        self.pass_on(a, block)

    def first_column_near(self):
        @pl.when(self.y == 1)
        def _():
            for a in self.each:
                self.take(a, self.up, 4)
            for a in self.each:
                self.take(a, self.cross, 6)
            for a in self.each:
                self.take(a, self.down, 3)
            for a in self.each:
                self.send(a, 5).start()

        @pl.when(self.y == 3)
        def _():
            for a in self.each:
                self.take(a, self.down, 3)
            for a in self.each:
                self.take(a, self.cross, 5)
            for a in self.each:
                self.take(a, self.up, 4)
            for a in self.each:
                self.send(a, 6).start()

        @pl.when(self.y % 2 == 0)
        def _():
            for a in self.each:
                self.take(a, self.down, 3)
                self.take(a, self.up, 4)
            for a in self.each:
                self.take(a, self.cross, 5, 6)

    def first_column_two(self):
        for a in self.each:
            self.got(a, self.two, 0)
            self.got(a, self.two, 1)
            self.pass_on(a, self.two)

    def first_column_cross(self):
        for a in self.each:
            self.take(a, self.cdown)
            self.take(a, self.cup)

    def first_column_far(self):
        for a in self.each:
            self.take(a, self.ctwo)

    def second_column(self):
        for a in self.each:
            self.take(a, self.down, 3)
            self.take(a, self.up, 4)
        for a in self.each:
            self.take(a, self.cross, 5, 6)
        for a in self.each:
            self.got(a, self.two, 0)
            self.got(a, self.two, 1)
            self.send(a, 7).start()
            self.pass_on(a, self.two)

        @pl.when(self.y == 1)
        def _():
            for a in self.each:
                self.take(a, self.cup, 9)
            for a in self.each:
                self.take(a, self.cdown, 8)

        @pl.when(self.y != 1)
        def _():
            for a in self.each:
                self.take(a, self.cdown, 8)
            for a in self.each:
                self.take(a, self.cup, 9)

    def second_column_far(self):
        for a in self.each:
            self.got(a, self.ctwo, 0, 2)
            self.got(a, self.ctwo, 1, 2)
            self.pass_on(a, self.ctwo)

    def phases(self, k):
        for phase, times in ((self.first_column_near, (1, 0, 0, 0, 9, 9, 9, 9)), (self.first_column_two, (2, 3, 0, 1, 9, 9, 9, 9)),
                             (self.first_column_cross, (5, 4, 4, 4, 9, 9, 9, 9)), (self.first_column_far, (6, 7, 4, 5, 9, 9, 9, 9)),
                             (self.second_column, (9, 9, 9, 9, 0, 0, 0, 0)), (self.second_column_far, (9, 9, 9, 9, 2, 3, 0, 1))):
            pl.when(table(self.seg, times) == k)(phase)

    def need(self, a, k):
        @pl.when(k != self.seg)
        def _():
            ref, base, n = self.parts[a]
            other = ref.at[k, pl.ds(pl.multiple_of(n - base, 8), n)]
            pltpu.make_async_remote_copy(
                src_ref=other, dst_ref=other, send_sem=self.dssem.at[a, k], recv_sem=self.dsem.at[a, k],
                device_id=self.sibling, device_id_type=MESH).wait_recv()

    def finish(self):
        for a in self.each:
            for i in range(7):
                self.send(a, i).wait_send()

            @pl.when(self.pair == 1)
            def _():
                for i in (7, 8, 9):
                    self.send(a, i).wait_send()
            if self.twins:
                for b in (self.down, self.up, self.cross, self.two, self.cdown, self.cup, self.ctwo):
                    self.twin(a, b).wait_send()


def entry_barrier():
    e = lax.axis_index("energy")
    seg = lax.axis_index("seg")
    core = e % 2
    pair, y = seg // 4, seg % 4
    barrier = pltpu.get_barrier_semaphore()

    def hello(to):
        pl.semaphore_signal(barrier, inc=1, device_id=to, device_id_type=MESH)

    for other in (pair * 4 + (y + 1) % 4, pair * 4 + (y + 3) % 4, (1 - pair) * 4 + y):
        hello({"seg": other})
    for d in range(1, 32):
        other = (e + d) % 32

        @pl.when((core == 1) | (other % 2 == 1))
        def _():
            hello({"energy": other})

    pl.semaphore_wait(barrier, 3 + 16 + 15 * core)


def identity():
    row = lax.broadcasted_iota(jnp.int32, (NB, NB), 0)
    col = lax.broadcasted_iota(jnp.int32, (NB, NB), 1)
    return (row == col).astype(f32)


def invert_into(L, s, x, el, rl, er, rr, br, fill=None):
    eye = identity()
    diag = x * eye
    d_col = 1.0 / jnp.sum(diag, axis=1, keepdims=True)
    d_row = 1.0 / jnp.sum(diag, axis=0, keepdims=True)
    e = eye - x * d_col
    put_left(el, e)
    put_right(er, e)
    if fill is not None:
        fill()
    r = mm(el, er)
    put_left(rl, r)
    put_right(rr, r)
    b = eye + e
    put_right(br, b)
    r = mm(rl, rr)
    b = b + mm(rl, br)
    put_left(el, r)
    put_right(er, r)
    put_right(br, b)
    r = mm(el, er)
    b = b + mm(el, br)
    put_left(rl, r)
    put_right(br, b)
    b = b + mm(rl, br)
    L[s] = b * d_row


def sweep(g, base_at, prepare, first, w, out):
    L, P, Q, C, CT, el, rl, er, rr, br, ql, ll = w
    seg = lax.axis_index("seg")
    g.phases(0)
    prepare(0)
    invert_into(L, 0, first(), el, rl, er, rr, br)

    def forward(k, carry):
        g.phases(k)
        prepare(k)
        left = L[k - 1]
        put_right(br, left)
        put_left(ll, left)
        q = mm(C.at[k], br)
        put_left(ql, q)
        put_right(Q.at[k], q)
        x = base_at(k) - mm(ql, CT.at[k])

        def fill():
            put_left(P.at[k], mm(ll, CT.at[k]))

        invert_into(L, k, x, el, rl, er, rr, br, fill)
        return carry

    lax.fori_loop(1, SEGS, forward, 0)
    out[...] = L[SEGS - 1]

    def backward(i, carry):
        t = SEGS - 1 - i
        put_right(br, out[...])
        put_left(el, mm(P.at[t], br))
        out[...] = L[t - 1] + mm(el, Q.at[t])
        return carry

    lax.fori_loop(0, SEGS - 1 - seg, backward, 0)


def exchange(green, off_ref, got, slabs, combined, out_ssem, out_rsem, back_ssem, back_rsem, meanwhile):
    e = lax.axis_index("energy")
    core, chip = e % 2, e // 2
    adder = core == 1

    rows = SLAB // PARTS

    def at(j, p):
        return pl.ds(pl.multiple_of(j * SLAB + p * rows, 8), rows)

    def out_copy(j, source, p):
        return pltpu.make_async_remote_copy(
            src_ref=green.at[at(j, p)], dst_ref=got[p].at[PAD + source],
            send_sem=out_ssem.at[p, j], recv_sem=out_rsem.at[p, source],
            device_id={"energy": 2 * j + 1}, device_id_type=MESH)

    def back_copy(energy, j, p):
        return pltpu.make_async_remote_copy(
            src_ref=slabs.at[energy, at(0, p)], dst_ref=combined.at[at(j, p)],
            send_sem=back_ssem.at[p, energy], recv_sem=back_rsem.at[p, j],
            device_id={"energy": energy}, device_id_type=MESH)

    def for_chips(body):
        for p in range(PARTS):
            def one(d, carry):
                j = (chip + d) % CHIPS

                @pl.when(e != 2 * j + 1)
                def _():
                    body(j, p)
                return carry
            lax.fori_loop(0, CHIPS, one, 0)

    for_chips(lambda j, p: out_copy(j, e, p).start())
    meanwhile()

    @pl.when(adder)
    def _():
        mine = pl.ds(pl.multiple_of(chip * SLAB, 8), SLAB)
        edge = jnp.zeros((rows, NB), f32)
        for p in range(PARTS):
            got[p][PAD + e] = green[at(chip, p)]
            for i in range(PAD):
                got[p][i] = edge
                got[p][PAD + ENERGIES + i] = edge
        o1, o2 = off_ref[0], off_ref[1]
        for p in range(PARTS):
            piece = pl.ds(p * rows, rows)

            def receive(d, carry):
                out_copy(chip, (e + d) % ENERGIES, p).wait_recv()
                return carry

            lax.fori_loop(1, ENERGIES, receive, 0)

            def add(i, carry):
                c = PAD + i
                slabs[i, piece] = got[p][c - o1] + got[p][c - o2] + got[p][c + o1] + got[p][c + o2]
                return carry

            lax.fori_loop(0, ENERGIES, add, 0)

            def send_back(d, carry):
                back_copy((e + d) % ENERGIES, chip, p).start()
                return carry

            lax.fori_loop(1, ENERGIES, send_back, 0)
        combined[mine] = slabs[e]

    for_chips(lambda j, p: back_copy(e, j, p).wait_recv())

    def finish():
        for_chips(lambda j, p: out_copy(j, e, p).wait_send())

        @pl.when(adder)
        def _():
            for p in range(PARTS):
                def sent_back(d, carry):
                    back_copy((e + d) % ENERGIES, chip, p).wait_send()
                    return carry

                lax.fori_loop(1, ENERGIES, sent_back, 0)

    return finish


def whole_kernel(lev_ref, off_ref, phi_ref, m_ref, c_ref, o_ref, se_ref,
                 cb, mb, sb, L, P, Q, C, CT, el, rl, er, rr, br, ql, ll, base0, green, got0, got1, got2, slabs, combined,
                 rsem, psem, ssem, dsem, dssem, rsem2, psem2, ssem2, out_ssem, out_rsem, back_ssem, back_rsem, lsem):
    seg = lax.axis_index("seg")
    own = [pltpu.make_async_copy(c_ref.at[0], cb.at[seg], lsem.at[0]),
           pltpu.make_async_copy(m_ref.at[0], mb.at[seg], lsem.at[1])]
    for c in own:
        c.start()
    entry_barrier()
    half = NB // 2
    mine = (lax.axis_index("energy") % 2) * half
    g = Gather(((cb, mine, half), (mb, mine, half)), rsem, psem, ssem, dsem, dssem)
    for a, c in enumerate(own):
        c.wait()
        g.start(a)
    for ref in (er, rr, br):
        clear_right(ref)
    w = (L, P, Q, C, CT, el, rl, er, rr, br, ql, ll)

    def prepare(k):
        clear_right(CT.at[k])
        clear_right(Q.at[k])
        g.need(0, k)
        g.need(1, k)
        c = cb[k]
        put_left(C.at[k], c)
        put_right(CT.at[k], c.T)

    def base_at(k):
        return mb[k] + lev_ref[0] * identity()

    def first():
        x = base_at(0) - 0.25 * mm(C.at[0], CT.at[0])
        base0[...] = x
        return x

    sweep(g, base_at, prepare, first, w, green)

    def meanwhile():
        phi = phi_ref[0]
        put_left(el, phi)
        put_right(rr, phi.T)

    finish = exchange(green, off_ref, (got0, got1, got2), slabs, combined, out_ssem, out_rsem, back_ssem, back_rsem, meanwhile)
    put_right(br, combined[...])
    put_left(ql, mm(el, br))
    sb[seg] = mm(ql, rr)
    third = NB // CUTS
    g2 = Gather([(sb, a * third, third) for a in range(CUTS)], rsem2, psem2, ssem2, None, None)
    for a in range(CUTS):
        g2.start(a)
    se_ref[...] = sb[seg]
    sweep(g2, lambda k: base_at(k) + sb[k], lambda k: None, lambda: base0[...] + sb[0], w, o_ref)
    finish()
    g.finish()
    g2.finish()


def block(n=None):
    return pltpu.VMEM((NB, NB) if n is None else (n, NB, NB), f32)


def left(*n):
    return pltpu.VMEM((*n, NB, 2 * NB), bf16)


def right(*n):
    return pltpu.VMEM((*n, 2 * NB, 2 * NB), bf16)


WORK = [block(8), left(8), right(8), left(8), right(8), left(), left(), right(), right(), right(), left(), left(), block()]
DMA = pltpu.SemaphoreType.DMA
VM = pl.BlockSpec(memory_space=pltpu.VMEM)
SM = pl.BlockSpec(memory_space=pltpu.SMEM)
ANY = pl.BlockSpec(memory_space=pl.ANY)
ONE = jax.ShapeDtypeStruct((NB, NB), f32)


def whole(levels, offsets, phonon, onsite, coupling):
    return pl.pallas_call(
        whole_kernel, out_shape=(ONE, ONE),
        in_specs=[SM, SM, VM, ANY, ANY], out_specs=(VM, VM),
        scratch_shapes=[block(8), block(8), block(8)] + WORK + [
            block(), *[pltpu.VMEM((ENERGIES + 2 * PAD, SLAB // PARTS, NB), f32)] * PARTS, pltpu.VMEM((ENERGIES, SLAB, NB), f32), block(),
            DMA((2, 8)), DMA((2, 4)), DMA((2, 10)), DMA((2, 8)), DMA((2, 8)),
            DMA((CUTS, 8)), DMA((CUTS, 4)), DMA((CUTS, 10)),
            DMA((PARTS, CHIPS)), DMA((PARTS, ENERGIES)), DMA((PARTS, ENERGIES)), DMA((PARTS, CHIPS)), DMA((2,))],
        compiler_params=pltpu.CompilerParams(vmem_limit_bytes=62 << 20, collective_id=0, has_side_effects=True),
        name="born",
    )(levels, offsets, phonon, onsite, coupling)


def shards(onsite, coupling, phonon, levels, offsets):
    green, self_energy = whole(levels, offsets, phonon, onsite, coupling)
    return green[None, None], self_energy[None, None]


def solution(mesh):
    spec = jax.sharding.PartitionSpec
    block_in = spec("seg", None, None)
    block_out = spec("energy", "seg", None, None)
    return jax.shard_map(shards, mesh=mesh, in_specs=(block_in, block_in, block_in, spec("energy"), spec()),
                         out_specs=(block_out, block_out), check_vma=False)
```

```python
import functools
import jax
import jax.numpy as jnp
from jax import lax
from jax.experimental import pallas as pl
from jax.experimental.pallas import tpu as pltpu

NB = 384
SEGS = 8
ENERGIES = 32
CHIPS = ENERGIES // 2
SLAB = NB // CHIPS
PAD = 15
PARTS = 3
RING = 8
ORDER = (12, 4, 11, 13, 3, 5, 10, 14, 2, 6, 9, 15, 1, 7, 8, 0)
HALVES = 2
CUTS = 3
f32 = jnp.float32
bf16 = jnp.bfloat16
MESH = pl.DeviceIdType.MESH


def split(x):
    hi = x.astype(bf16)
    lo = (x - hi.astype(f32)).astype(bf16)
    return hi, lo


def put_left(ref, x):
    hi, lo = split(x)
    ref[:, 0:256] = hi[:, 0:256]
    ref[:, 256:512] = lo[:, 0:256]
    ref[:, 512:640] = hi[:, 256:384]
    ref[:, 640:768] = lo[:, 256:384]


def put_right(ref, x):
    hi, lo = split(x)
    ref[0:256, 0:384] = hi[0:256]
    ref[256:512, 0:384] = hi[0:256]
    ref[0:256, 384:768] = lo[0:256]
    ref[512:640, 0:384] = hi[256:384]
    ref[640:768, 0:384] = hi[256:384]
    ref[512:640, 384:768] = lo[256:384]


def clear_right(ref):
    ref[256:512, 384:768] = jnp.zeros((256, 384), bf16)
    ref[640:768, 384:768] = jnp.zeros((128, 384), bf16)


def dot(a, b):
    return lax.dot_general(a, b, (((1,), (0,)), ((), ())), preferred_element_type=f32)


def mm(l, r, which=None):
    out = []
    for h in range(HALVES) if which is None else (which,):
        n = NB // HALVES
        rows = slice(h * n, h * n + n)
        a = dot(l[rows, :], r[:, 0:512])
        b = dot(l[rows, 0:256], r[0:256, 512:768]) + dot(l[rows, 512:768], r[512:768, 512:768])
        out.append(jnp.concatenate([a[:, 0:128] + a[:, 384:512], a[:, 128:384] + b], axis=1))
    return jnp.concatenate(out, axis=0)


def table(seg, values):
    out = jnp.int32(values[-1])
    for i, v in enumerate(values[:-1]):
        out = jnp.where(seg == i, jnp.int32(v), out)
    return out


class Gather:
    def __init__(self, parts, rsem, psem, ssem, dsem, dssem):
        self.parts, self.rsem, self.psem, self.ssem, self.dsem, self.dssem = parts, rsem, psem, ssem, dsem, dssem
        self.each = range(len(parts))
        self.twins = dsem is not None
        e = lax.axis_index("energy")
        self.seg = lax.axis_index("seg")
        self.sibling = {"energy": e + 1 - 2 * (e % 2)}
        self.pair, self.y = self.seg // 4, self.seg % 4
        at = lambda p, dy: p * 4 + (self.y + dy) % 4
        self.up, self.down, self.two = at(self.pair, 1), at(self.pair, 3), at(self.pair, 2)
        other = 1 - self.pair
        self.cross, self.cup, self.cdown, self.ctwo = at(other, 0), at(other, 1), at(other, 3), at(other, 2)

    def view(self, a, block, part=None):
        ref, base, n = self.parts[a]
        if part is not None:
            n = n // 2
            base = base + part * n
        return ref.at[block, pl.ds(pl.multiple_of(base, 8), n)]

    def copy(self, a, block, part, s, sem, to):
        ref = self.view(a, block, part)
        return pltpu.make_async_remote_copy(
            src_ref=ref, dst_ref=ref, send_sem=self.ssem.at[a, s], recv_sem=sem,
            device_id=to, device_id_type=MESH)

    def got(self, a, block, part=None):
        sem = self.rsem.at[a, block] if part is None else self.psem.at[a, part]
        self.copy(a, block, part, 0, sem, {"seg": self.up}).wait_recv()

    def send(self, a, i):
        r, p = self.rsem, self.psem
        up, down, cross = {"seg": self.up}, {"seg": self.down}, {"seg": self.cross}
        block, part, sem, to = (
            (self.seg, None, r.at[a, self.seg], up),
            (self.seg, None, r.at[a, self.seg], down),
            (self.seg, None, r.at[a, self.seg], cross),
            (self.down, 0, p.at[a, 0], up),
            (self.up, 1, p.at[a, 1], down),
            (self.cross, None, r.at[a, self.cross], up),
            (self.cross, None, r.at[a, self.cross], down),
            (self.two, None, r.at[a, self.two], cross),
        )[i]
        return self.copy(a, block, part, i, sem, to)

    def twin(self, a, block):
        ref = self.view(a, block)
        return pltpu.make_async_remote_copy(
            src_ref=ref, dst_ref=ref, send_sem=self.dssem.at[a, block], recv_sem=self.dsem.at[a, block],
            device_id=self.sibling, device_id_type=MESH)

    def pass_on(self, a, block):
        if self.twins:
            self.twin(a, block).start()

    def start(self, a):
        for i in range(3):
            self.send(a, i).start()

    def take(self, a, block, *sends):
        self.got(a, block)
        for i in sends:
            self.send(a, i).start()
        self.pass_on(a, block)

    def phase1(self):
        for a in self.each:
            self.take(a, self.down, 3)
            self.take(a, self.up, 4)
        for a in self.each:
            self.take(a, self.cross, 5, 6)

    def phase2(self):
        for a in self.each:
            self.got(a, self.two, 0)
            self.got(a, self.two, 1)
            self.send(a, 7).start()
            self.pass_on(a, self.two)

    def phase3(self):
        for a in self.each:
            for b in (self.cdown, self.cup):
                self.take(a, b)

    def phase4(self):
        for a in self.each:
            self.take(a, self.ctwo)

    def phases(self, k):
        for phase, times in ((self.phase1, (1, 0, 0, 0, 0, 0, 0, 0)), (self.phase2, (2, 3, 0, 1, 1, 0, 0, 0)),
                             (self.phase3, (5, 4, 4, 4, 1, 0, 0, 0)), (self.phase4, (6, 7, 4, 5, 2, 3, 0, 1))):
            pl.when(table(self.seg, times) == k)(phase)

    def need(self, a, k):
        @pl.when(k != self.seg)
        def _():
            ref, base, n = self.parts[a]
            other = ref.at[k, pl.ds(pl.multiple_of(n - base, 8), n)]
            pltpu.make_async_remote_copy(
                src_ref=other, dst_ref=other, send_sem=self.dssem.at[a, k], recv_sem=self.dsem.at[a, k],
                device_id=self.sibling, device_id_type=MESH).wait_recv()

    def finish(self):
        for a in self.each:
            for i in range(8):
                self.send(a, i).wait_send()
            if self.twins:
                for b in (self.down, self.up, self.cross, self.two, self.cdown, self.cup, self.ctwo):
                    self.twin(a, b).wait_send()


def entry_barrier():
    e = lax.axis_index("energy")
    seg = lax.axis_index("seg")
    core = e % 2
    pair, y = seg // 4, seg % 4
    barrier = pltpu.get_barrier_semaphore()

    def hello(to):
        pl.semaphore_signal(barrier, inc=1, device_id=to, device_id_type=MESH)

    for other in (pair * 4 + (y + 1) % 4, pair * 4 + (y + 3) % 4, (1 - pair) * 4 + y):
        hello({"seg": other})
    for d in range(1, 32):
        other = (e + d) % 32

        @pl.when((core == 1) | (other % 2 == 1))
        def _():
            hello({"energy": other})

    pl.semaphore_wait(barrier, 3 + 16 + 15 * core)


def identity():
    row = lax.broadcasted_iota(jnp.int32, (NB, NB), 0)
    col = lax.broadcasted_iota(jnp.int32, (NB, NB), 1)
    return (row == col).astype(f32)


def invert_into(L, s, x, el, rl, er, rr, br, fill=None):
    eye = identity()
    diag = x * eye
    d_col = 1.0 / jnp.sum(diag, axis=1, keepdims=True)
    d_row = 1.0 / jnp.sum(diag, axis=0, keepdims=True)
    e = eye - x * d_col
    put_left(el, e)
    put_right(er, e)
    if fill is not None:
        fill(0)
    r = mm(el, er)
    if fill is not None:
        fill(1)
    put_left(rl, r)
    put_right(rr, r)
    b = eye + e
    put_right(br, b)
    r = mm(rl, rr)
    b = b + mm(rl, br)
    put_left(el, r)
    put_right(er, r)
    put_right(br, b)
    r = mm(el, er)
    b = b + mm(el, br)
    put_left(rl, r)
    put_right(br, b)
    b = b + mm(rl, br)
    L[s] = b * d_row


def sweep(g, base_at, prepare, first, w, out):
    L, P, Q, C, CT, el, rl, er, rr, br, ql, ll = w
    seg = lax.axis_index("seg")
    g.phases(0)
    prepare(0)
    invert_into(L, 0, first(), el, rl, er, rr, br)

    def forward(k, carry):
        g.phases(k)
        prepare(k)
        left = L[k - 1]
        put_right(br, left)
        put_left(ll, left)
        q = mm(C.at[k], br)
        put_left(ql, q)
        put_right(Q.at[k], q)
        x = base_at(k) - mm(ql, CT.at[k])

        def fill(h):
            put_left(P.at[k, pl.ds(h * (NB // HALVES), NB // HALVES)], mm(ll, CT.at[k], h))

        invert_into(L, k, x, el, rl, er, rr, br, fill)
        return carry

    lax.fori_loop(1, SEGS, forward, 0)
    out[...] = L[SEGS - 1]

    def backward(i, carry):
        t = SEGS - 1 - i
        put_right(br, out[...])
        put_left(el, mm(P.at[t], br))
        out[...] = L[t - 1] + mm(el, Q.at[t])
        return carry

    lax.fori_loop(0, SEGS - 1 - seg, backward, 0)


def exchange(green, off_ref, got, slabs, combined, out_ssem, out_rsem, back_ssem, back_rsem, meanwhile):
    e = lax.axis_index("energy")
    core, chip = e % 2, e // 2
    adder = core == 1

    rows = SLAB // PARTS

    def at(j, p):
        return pl.ds(pl.multiple_of(j * SLAB + p * rows, 8), rows)

    def out_copy(j, source, p):
        return pltpu.make_async_remote_copy(
            src_ref=green.at[at(j, p)], dst_ref=got[p].at[PAD + source],
            send_sem=out_ssem.at[p, j], recv_sem=out_rsem.at[p, source],
            device_id={"energy": 2 * j + 1}, device_id_type=MESH)

    def back_copy(energy, j, p):
        return pltpu.make_async_remote_copy(
            src_ref=slabs.at[energy, at(0, p)], dst_ref=combined.at[at(j, p)],
            send_sem=back_ssem.at[p, energy], recv_sem=back_rsem.at[p, j],
            device_id={"energy": energy}, device_id_type=MESH)

    def chip_at(d):
        return (chip // RING + d // RING) % 2 * RING + (chip + d) % RING

    def for_chips(body):
        for p in range(PARTS):
            for d in ORDER:
                j = chip_at(d)

                @pl.when(e != 2 * j + 1)
                def _():
                    body(j, p)

    for_chips(lambda j, p: out_copy(j, e, p).start())
    meanwhile()

    @pl.when(adder)
    def _():
        mine = pl.ds(pl.multiple_of(chip * SLAB, 8), SLAB)
        edge = jnp.zeros((rows, NB), f32)
        for p in range(PARTS):
            got[p][PAD + e] = green[at(chip, p)]
            for i in range(PAD):
                got[p][i] = edge
                got[p][PAD + ENERGIES + i] = edge
        o1, o2 = off_ref[0], off_ref[1]
        for p in range(PARTS):
            piece = pl.ds(p * rows, rows)

            def receive(d, carry):
                out_copy(chip, (e + d) % ENERGIES, p).wait_recv()
                return carry

            lax.fori_loop(1, ENERGIES, receive, 0)

            def add(i, carry):
                c = PAD + i
                slabs[i, piece] = got[p][c - o1] + got[p][c - o2] + got[p][c + o1] + got[p][c + o2]
                return carry

            lax.fori_loop(0, ENERGIES, add, 0)

            for d in ORDER:
                back_copy(2 * chip_at(d), chip, p).start()
                if d:
                    back_copy(2 * chip_at(d) + 1, chip, p).start()
        combined[mine] = slabs[e]

    for_chips(lambda j, p: back_copy(e, j, p).wait_recv())

    def finish():
        for_chips(lambda j, p: out_copy(j, e, p).wait_send())

        @pl.when(adder)
        def _():
            for p in range(PARTS):
                def sent_back(d, carry):
                    back_copy((e + d) % ENERGIES, chip, p).wait_send()
                    return carry

                lax.fori_loop(1, ENERGIES, sent_back, 0)

    return finish


def whole_kernel(lev_ref, off_ref, phi_ref, m_ref, c_ref, o_ref, se_ref,
                 cb, mb, sb, L, P, Q, C, CT, el, rl, er, rr, br, ql, ll, base0, green, got0, got1, got2, slabs, combined,
                 rsem, psem, ssem, dsem, dssem, rsem2, psem2, ssem2, out_ssem, out_rsem, back_ssem, back_rsem, lsem):
    seg = lax.axis_index("seg")
    own = [pltpu.make_async_copy(c_ref.at[0], cb.at[seg], lsem.at[0]),
           pltpu.make_async_copy(m_ref.at[0], mb.at[seg], lsem.at[1])]
    for c in own:
        c.start()
    entry_barrier()
    half = NB // 2
    mine = (lax.axis_index("energy") % 2) * half
    g = Gather(((cb, mine, half), (mb, mine, half)), rsem, psem, ssem, dsem, dssem)
    for a, c in enumerate(own):
        c.wait()
        g.start(a)
    for ref in (er, rr, br):
        clear_right(ref)
    w = (L, P, Q, C, CT, el, rl, er, rr, br, ql, ll)

    def prepare(k):
        clear_right(CT.at[k])
        clear_right(Q.at[k])
        g.need(0, k)
        g.need(1, k)
        c = cb[k]
        put_left(C.at[k], c)
        put_right(CT.at[k], c.T)

    def base_at(k):
        return mb[k] + lev_ref[0] * identity()

    def first():
        x = base_at(0) - 0.25 * mm(C.at[0], CT.at[0])
        base0[...] = x
        return x

    sweep(g, base_at, prepare, first, w, green)

    def meanwhile():
        phi = phi_ref[0]
        put_left(el, phi)
        put_right(rr, phi.T)

    finish = exchange(green, off_ref, (got0, got1, got2), slabs, combined, out_ssem, out_rsem, back_ssem, back_rsem, meanwhile)
    put_right(br, combined[...])
    put_left(ql, mm(el, br))
    sb[seg] = mm(ql, rr)
    third = NB // CUTS
    g2 = Gather([(sb, a * third, third) for a in range(CUTS)], rsem2, psem2, ssem2, None, None)
    for a in range(CUTS):
        g2.start(a)
    se_ref[...] = sb[seg]
    sweep(g2, lambda k: base_at(k) + sb[k], lambda k: None, lambda: base0[...] + sb[0], w, o_ref)
    finish()
    g.finish()
    g2.finish()


def block(n=None):
    return pltpu.VMEM((NB, NB) if n is None else (n, NB, NB), f32)


def left(*n):
    return pltpu.VMEM((*n, NB, 2 * NB), bf16)


def right(*n):
    return pltpu.VMEM((*n, 2 * NB, 2 * NB), bf16)


WORK = [block(8), left(8), right(8), left(8), right(8), left(), left(), right(), right(), right(), left(), left(), block()]
DMA = pltpu.SemaphoreType.DMA
VM = pl.BlockSpec(memory_space=pltpu.VMEM)
SM = pl.BlockSpec(memory_space=pltpu.SMEM)
ANY = pl.BlockSpec(memory_space=pl.ANY)
ONE = jax.ShapeDtypeStruct((NB, NB), f32)


def whole(levels, offsets, phonon, onsite, coupling):
    return pl.pallas_call(
        whole_kernel, out_shape=(ONE, ONE),
        in_specs=[SM, SM, VM, ANY, ANY], out_specs=(VM, VM),
        scratch_shapes=[block(8), block(8), block(8)] + WORK + [
            block(), *[pltpu.VMEM((ENERGIES + 2 * PAD, SLAB // PARTS, NB), f32)] * PARTS, pltpu.VMEM((ENERGIES, SLAB, NB), f32), block(),
            DMA((2, 8)), DMA((2, 2)), DMA((2, 8)), DMA((2, 8)), DMA((2, 8)),
            DMA((CUTS, 8)), DMA((CUTS, 2)), DMA((CUTS, 8)),
            DMA((PARTS, CHIPS)), DMA((PARTS, ENERGIES)), DMA((PARTS, ENERGIES)), DMA((PARTS, CHIPS)), DMA((2,))],
        compiler_params=pltpu.CompilerParams(vmem_limit_bytes=62 << 20, collective_id=0, has_side_effects=True),
        name="born",
    )(levels, offsets, phonon, onsite, coupling)


def shards(onsite, coupling, phonon, levels, offsets):
    green, self_energy = whole(levels, offsets, phonon, onsite, coupling)
    return green[None, None], self_energy[None, None]


def solution(mesh):
    spec = jax.sharding.PartitionSpec
    block_in = spec("seg", None, None)
    block_out = spec("energy", "seg", None, None)
    return jax.shard_map(shards, mesh=mesh, in_specs=(block_in, block_in, block_in, spec("energy"), spec()),
                         out_specs=(block_out, block_out), check_vma=False)
```
